32 devices in a mesh: dp: 4 (over z), seq: 8 (over y, x, core).
Axes of the slice: x: 2, y: 2, z: 4, core: 2. Of those that a mesh axis runs over, the one named last changes fastest.
Arguments:
- hidden_in: bfloat16 [8, 1024, 2048], P('dp', 'seq'), may hold values from -6 to 6
- w_qkv: float32 [2048, 1920], P(('dp', 'seq')), may hold values from -0.125 to 0.125
- w_out: float32 [1280, 2048], P(('dp', 'seq')), may hold values from -1.25 to 1.25
- w_gate_up: float32 [2048, 16384], P(('dp', 'seq')), may hold values from -0.125 to 0.125
- w_down: float32 [8192, 2048], P(('dp', 'seq')), may hold values from -0.0625 to 0.0625
- norm_gains: float32 [4224], P(('dp', 'seq')), may hold values from 0.25 to 1.75
- segment_ids: int32 [8, 1024], P('dp', 'seq'), may hold values from 0 to 7, as said below
- positions: int32 [8, 1024], P('dp', 'seq'), may hold values from 0 to 1023, as said below
- out_grad: bfloat16 [8, 1024, 2048], P('dp', 'seq'), may hold values from -6 to 6
Outputs:
- block_out: bfloat16 [8, 1024, 2048], P('dp', 'seq')
- in_grad: bfloat16 [8, 1024, 2048], P('dp', 'seq')
- grad_qkv: float32 [2048, 1920], P(('dp', 'seq'))
- grad_out: float32 [1280, 2048], P(('dp', 'seq'))
- grad_gate_up: float32 [2048, 16384], P(('dp', 'seq'))
- grad_down: float32 [8192, 2048], P(('dp', 'seq'))
- grad_gains: float32 [4224], P(('dp', 'seq'))
The draws below stay inside these ranges and needn't reach their ends.
Inputs may be any that keep to these rules, and one draw needn't show every extreme that they name: `segment_ids`: in each row the ids start at 0, never fall, and rise by one where a document starts; row 0 is a single document, every other row holds exactly 8 documents. `positions`: A token's position is its distance from the first token of its document in the row.
All inputs are finite; a program needn't handle non-finite values.
Results may differ from the reference program's by a relative error of at most 0.015.
The reference program's roundings to bfloat16 on the way count: a program that leaves them out, or rounds other values in their place, can miss the bound.
Values may be sent and summed in bfloat16 or wider, within the bound.
A program may use at most 448 MiB of HBM per device.

```python
import jax
import jax.numpy as jnp
from jax import lax

D = 2048
QUERY_HEADS = 20
KEY_VALUE_HEADS = 5
HEAD_SIZE = 64
FF = 8192
ROWS = 8
ROW_LENGTH = 1024
QUERIES_PER_KEY = 4
QKV = 1920
GAINS = 4224


def documents(key):
    marker_key = jax.random.fold_in(key, 17)
    row_keys = jax.random.split(marker_key, ROWS)
    orders = jax.vmap(lambda row_key: jax.random.permutation(row_key, ROW_LENGTH - 1))(row_keys)
    chosen = (orders[:, :7] + 1).astype(jnp.int32)
    column = jnp.arange(ROW_LENGTH, dtype=jnp.int32)[None, :]
    row_ids = jnp.arange(ROWS, dtype=jnp.int32)[:, None]
    marks = jnp.any(column[:, :, None] == chosen[:, None, :], axis=-1)
    marks = marks & (row_ids > 0)
    segment = jnp.cumsum(marks.astype(jnp.int32), axis=1).astype(jnp.int32)
    starts = lax.cummax(jnp.where(marks, column, 0).astype(jnp.int32), axis=1)
    return (segment, (column - starts).astype(jnp.int32))


def draw_segment_ids(key, part):
    return documents(key)[0]


def draw_positions(key, part):
    return documents(key)[1]


def level_of(key, extent, shards, least, high):
    level, own = 1.0, jax.random.fold_in(key, 6)
    for position, shards_of in shards:
        steps = jnp.exp(jax.random.uniform(jax.random.fold_in(own, position), (shards_of,), jnp.float32, least / len(shards), high / len(shards)))
        level = level * jnp.repeat(steps, extent[position] // shards_of).reshape([-1 if axis == position else 1 for axis in range(len(extent))])
    return level


def scatter_about(rng, dims, deviation, limit, cuts=(), held_as=jnp.bfloat16):
    entries = jax.random.normal(rng, dims, jnp.float32) * deviation
    if len(cuts) > 0:
        entries = level_of(rng, dims, cuts, -0.22, 0.18) * entries
    return jnp.clip(entries, min=-limit, max=limit).astype(held_as)


def setup_inputs(seed: int = 0) -> dict:
    keys = jax.random.split(jax.random.key(seed), 10)
    return {
        "hidden_in": scatter_about(keys[0], (ROWS, ROW_LENGTH, D), 1.0, 6.0, ((0, 4), (1, 8))),
        "w_qkv": scatter_about(keys[1], (D, QKV), D ** -0.5, 0.125, ((0, 32),), jnp.float32),
        "w_out": scatter_about(keys[2], (QUERY_HEADS * HEAD_SIZE, D), (QUERY_HEADS * HEAD_SIZE // 64) ** -0.5, 1.25, ((0, 32),), jnp.float32),
        "w_gate_up": scatter_about(keys[3], (D, 2 * FF), D ** -0.5, 0.125, ((0, 32),), jnp.float32),
        "w_down": scatter_about(keys[4], (FF, D), FF ** -0.5, 0.0625, ((0, 32),), jnp.float32),
        "norm_gains": jnp.clip(1.0 + 0.15 * jax.random.normal(keys[5], (GAINS,), jnp.float32), 0.25, 1.75),
        "segment_ids": draw_segment_ids(jax.random.fold_in(keys[9], 71), 0),
        "positions": draw_positions(jax.random.fold_in(keys[9], 71), 0),
        "out_grad": scatter_about(keys[8], (ROWS, ROW_LENGTH, D), 1.0, 6.0, ((0, 4), (1, 8))),
    }


EPSILON = 1e-06
MASKED = -1e+30
HIGHEST = lax.Precision.HIGHEST

@jax.custom_vjp
def reduced_precision(v):
    return lax.optimization_barrier(v.astype(jnp.bfloat16)).astype(jnp.float32)

@jax.custom_vjp
def low_back(v):
    return v

def low_keep(v):
    return (reduced_precision(v), None)

def low_pass(kept, grad):
    return (grad,)

def back_keep(v):
    return (v, None)

def back_low(kept, grad):
    return (reduced_precision(grad),)
reduced_precision.defvjp(low_keep, low_pass)
low_back.defvjp(back_keep, back_low)

def norm_rows(values, gain_vec):
    return values * lax.rsqrt(lax.optimization_barrier(jnp.mean(values * values, axis=-1, keepdims=True)) + EPSILON) * gain_vec

def apply_rotation(values, cosine_table, sine_table):
    half_dim = values.shape[-1] // 2
    first, second = (values[..., :half_dim], values[..., half_dim:])
    return jnp.concatenate([first * cosine_table - second * sine_table, second * cosine_table + first * sine_table], axis=-1)

def rope_tables(position_row):
    freq = 1.0 / 10000.0 ** (jnp.arange(0, HEAD_SIZE, 2).astype(jnp.float32) / HEAD_SIZE)
    angle = position_row.astype(jnp.float32)[:, None] * freq[None, :]
    return (jnp.cos(angle)[:, None, :], jnp.sin(angle)[:, None, :])

def reference(hidden_in, w_qkv, w_out, w_gate_up, w_down, norm_gains, segment_ids, positions, out_grad):
    scale = HEAD_SIZE ** (-0.5)
    tok_index = jnp.arange(ROW_LENGTH)
    causal = tok_index[:, None] >= tok_index[None, :]

    def layer(inputs, wq_in, wo_in, wg_in, wd_in, gains_in):
        w_query = reduced_precision(wq_in)
        w_proj = reduced_precision(wo_in)
        w_gate = reduced_precision(wg_in)
        w_drop = reduced_precision(wd_in)
        gains = reduced_precision(gains_in)
        gain_one = gains[:D]
        gain_two = gains[D:2 * D]
        gain_query = gains[2 * D:2 * D + HEAD_SIZE]
        key_gain_vector = gains[2 * D + HEAD_SIZE:]

        def one_row(row_args):
            row_vals, seg_row, pos_row = row_args
            normed = reduced_precision(norm_rows(row_vals, gain_one))
            query_key_value_output = low_back(jnp.dot(normed, w_query, precision=HIGHEST))
            cosine_table, sine_table = rope_tables(pos_row)
            query_rows = query_key_value_output[:, :QUERY_HEADS * HEAD_SIZE].reshape(ROW_LENGTH, QUERY_HEADS, HEAD_SIZE)
            unrotated_keys = query_key_value_output[:, QUERY_HEADS * HEAD_SIZE:(QUERY_HEADS + KEY_VALUE_HEADS) * HEAD_SIZE].reshape(ROW_LENGTH, KEY_VALUE_HEADS, HEAD_SIZE)
            value_rows = reduced_precision(query_key_value_output[:, (QUERY_HEADS + KEY_VALUE_HEADS) * HEAD_SIZE:].reshape(ROW_LENGTH, KEY_VALUE_HEADS, HEAD_SIZE))
            query_rows = reduced_precision(apply_rotation(norm_rows(query_rows, gain_query), cosine_table, sine_table))
            rotated_keys = reduced_precision(apply_rotation(norm_rows(unrotated_keys, key_gain_vector), cosine_table, sine_table))
            allowed = causal & (seg_row[:, None] == seg_row[None, :])

            def single_head(head_args):
                q_head, k_head, v_head = head_args
                scores = low_back(jnp.einsum('qgd,kd->gqk', q_head, k_head, precision=HIGHEST) * scale)
                scores = jnp.where(allowed[None], scores, MASKED)
                row_peak = lax.optimization_barrier(jnp.max(scores, axis=-1, keepdims=True))
                shifted = jnp.exp(scores - row_peak)
                probs = reduced_precision(shifted / lax.optimization_barrier(jnp.sum(shifted, axis=-1, keepdims=True)))
                return jnp.einsum('gqk,kd->qgd', probs, v_head, precision=HIGHEST)
            head_list = lax.map(jax.checkpoint(single_head), (query_rows.reshape(ROW_LENGTH, KEY_VALUE_HEADS, QUERIES_PER_KEY, HEAD_SIZE).transpose(1, 0, 2, 3), rotated_keys.transpose(1, 0, 2), value_rows.transpose(1, 0, 2)))
            attended = head_list.transpose(1, 0, 2, 3).reshape(ROW_LENGTH, QUERY_HEADS * HEAD_SIZE)
            attended = reduced_precision(low_back(attended))
            mixed = row_vals + low_back(jnp.dot(attended, w_proj, precision=HIGHEST))
            normed_two = reduced_precision(norm_rows(mixed, gain_two))
            gate_up = low_back(jnp.dot(normed_two, w_gate, precision=HIGHEST))
            gate_part = gate_up[:, :FF]
            hidden = reduced_precision(gate_part * jax.nn.sigmoid(gate_part) * gate_up[:, FF:])
            return mixed + jnp.dot(hidden, w_drop, precision=HIGHEST)
        return lax.map(jax.checkpoint(one_row), (inputs, segment_ids, positions))
    result, pullback = jax.vjp(layer, hidden_in.astype(jnp.float32), w_qkv, w_out, w_gate_up, w_down, norm_gains)
    grads = pullback(out_grad.astype(jnp.float32))
    return (result.astype(jnp.bfloat16), grads[0].astype(jnp.bfloat16), grads[1], grads[2], grads[3], grads[4], grads[5])
```

```python
import functools

import jax
import jax.numpy as jnp
from jax import lax
from jax.experimental import pallas as pl
from jax.experimental.pallas import tpu as pltpu
from jax.sharding import PartitionSpec as P

D = 2048
QUERY_HEADS = 20
KEY_VALUE_HEADS = 5
HEAD_SIZE = 64
FF = 8192
GROUP = QUERY_HEADS // KEY_VALUE_HEADS
QUERY_WIDTH = QUERY_HEADS * HEAD_SIZE
PAIR_WIDTH = 2 * HEAD_SIZE
KV_WIDTH = KEY_VALUE_HEADS * PAIR_WIDTH
GROUP_WIDTH = GROUP * HEAD_SIZE

EPSILON = 1e-06
MASKED = -1e30
SCALE = HEAD_SIZE ** (-0.5)


def normalized_rows(values):
    scale_rows = lax.rsqrt(jnp.mean(values * values, axis=-1, keepdims=True) + EPSILON)
    return (values * scale_rows, scale_rows)


def normalized_gradient(upstream, unit_vals, scale_rows):
    return scale_rows * (
        upstream - unit_vals * jnp.mean(upstream * unit_vals, axis=-1, keepdims=True)
    )


def apply_rotation(values, cosine_table, sine_table):
    half_dim = values.shape[-1] // 2
    first, second = (values[..., :half_dim], values[..., half_dim:])
    return jnp.concatenate(
        [first * cosine_table - second * sine_table, second * cosine_table + first * sine_table],
        axis=-1,
    )


def rope_tables(position_flat):
    freq = 1.0 / 10000.0 ** (jnp.arange(0, HEAD_SIZE, 2).astype(jnp.float32) / HEAD_SIZE)
    angle = position_flat.astype(jnp.float32)[:, None] * freq[None, :]
    return (jnp.cos(angle)[:, None, :], jnp.sin(angle)[:, None, :])


def matmul(left, right):
    return jnp.dot(left, right, preferred_element_type=jnp.float32)


def contract_rows(left, right):
    return lax.dot_general(
        left, right, (((0,), (0,)), ((), ())), preferred_element_type=jnp.float32
    )


def contract_cols(left, right):
    return lax.dot_general(
        left, right, (((1,), (1,)), ((), ())), preferred_element_type=jnp.float32
    )


def shifted(piece, shift):
    count = lax.axis_size("dp")
    return lax.ppermute(piece, "dp", [(i, (i + shift) % count) for i in range(count)])


def rotate_gather(piece):
    return [piece] + [shifted(piece, s) for s in range(1, lax.axis_size("dp"))]


def rotate_reduce(partial, rows):
    total = partial[:rows].astype(jnp.float32)
    for s in range(1, lax.axis_size("dp")):
        piece = partial[s * rows : (s + 1) * rows].astype(jnp.bfloat16)
        total = total + shifted(piece, -s).astype(jnp.float32)
    return total


def in_order(slots):
    count = len(slots)
    back = slots[::-1] + slots[::-1]
    start = count - 1 - lax.axis_index("dp")
    return lax.dynamic_slice_in_dim(jnp.stack(back[:-1]), start, count, axis=0)


def exchange_blocks(blocks):
    count = lax.axis_size("dp")
    me = lax.axis_index("dp")
    pick = lambda s: lax.dynamic_index_in_dim(blocks, lax.rem(me + s, count), 0, keepdims=False)
    return in_order([pick(0)] + [shifted(pick(s), s) for s in range(1, count)])


def reduce_blocks(blocks):
    count = lax.axis_size("dp")
    me = lax.axis_index("dp")
    pick = lambda s: lax.dynamic_index_in_dim(blocks, lax.rem(me + s, count), 0, keepdims=False)
    total = pick(0).astype(jnp.float32)
    for s in range(1, count):
        total = total + shifted(pick(s), s).astype(jnp.float32)
    return total


def bit_orders(count, ways):
    bits = [1 << i for i in range(1, count.bit_length() - 1)]
    half = (len(bits) + 1) // 2
    low, high = bits[:half], bits[half:]
    orders = []
    for way in range(ways):
        one, two = (low, high) if way % 2 == 0 else (high, low)
        order = []
        for i in range(half):
            order += one[i : i + 1] + two[i : i + 1]
        orders.append(tuple(order + [1]))
    return orders


def crossed(piece, bit):
    count = lax.axis_size("seq")
    return lax.ppermute(piece, "seq", [(i, i ^ bit) for i in range(count)])


def cube_gather(piece, bits):
    for bit in bits:
        piece = jnp.concatenate([piece, crossed(piece, bit)], axis=0)
    return piece


def cube_offsets(bits):
    offsets = [0]
    for bit in bits:
        offsets = offsets + [o ^ bit for o in offsets]
    return tuple(offsets)


def cube_reduce(partial, bits):
    for bit in bits[::-1]:
        half = partial.shape[0] // 2
        partial = partial[:half].astype(jnp.float32) + crossed(
            partial[half:].astype(jnp.bfloat16), bit
        ).astype(jnp.float32)
    return partial


def fill_bias(place_ref, start_ref, bias_ref, offsets):
    rows = start_ref.shape[1]
    place = place_ref[0]
    query = place * rows + lax.broadcasted_iota(jnp.int32, (rows, rows), 1)
    begin = start_ref[...]
    local = lax.broadcasted_iota(jnp.int32, (rows, rows), 0)
    for slot, offset in enumerate(offsets):
        key = (place ^ offset) * rows + local
        allowed = (key <= query) & (key >= begin)
        bias_ref[slot * rows : (slot + 1) * rows, :] = jnp.where(allowed, 0.0, MASKED)


def stacked_heads(block, place):
    rows = block.shape[0]
    turned = block.astype(jnp.float32).T
    heads = jnp.concatenate(
        [turned[g * HEAD_SIZE : (g + 1) * HEAD_SIZE] for g in range(GROUP)], axis=1
    ).astype(jnp.bfloat16)
    empty = jnp.zeros((HEAD_SIZE, GROUP * rows), jnp.bfloat16)
    return jnp.concatenate([heads, empty] if place == 0 else [empty, heads], axis=0)


def unstacked_heads(turned):
    rows = turned.shape[1] // GROUP
    return jnp.concatenate([turned[:, g * rows : (g + 1) * rows] for g in range(GROUP)], axis=0).T


def attend_kernel(offsets, place_ref, start_ref, q_ref, kv_ref, out_ref, lse_ref, bias_ref):
    @pl.when(pl.program_id(0) == 0)
    def _():
        fill_bias(place_ref, start_ref, bias_ref, offsets)

    pairs = kv_ref[...]
    queries = stacked_heads(q_ref[...], 0)
    bias = jnp.concatenate([bias_ref[...]] * GROUP, axis=1)
    scores = matmul(pairs, queries) + bias
    peak = jnp.max(scores, axis=0, keepdims=True)
    raised = jnp.exp(scores - peak)
    totals = jnp.sum(raised, axis=0, keepdims=True)
    probs = (raised * (1.0 / totals)).astype(jnp.bfloat16)
    mixed = contract_rows(pairs, probs)
    out_ref[...] = unstacked_heads(mixed[HEAD_SIZE:]).astype(jnp.bfloat16)
    lse_ref[0] = peak + jnp.log(totals)


def attend_back_kernel(
    offsets, place_ref, start_ref, q_ref, kv_ref, do_ref, lse_ref, dq_ref, dkv_ref, bias_ref
):
    @pl.when(pl.program_id(0) == 0)
    def _():
        fill_bias(place_ref, start_ref, bias_ref, offsets)

    pairs = kv_ref[...]
    queries = stacked_heads(q_ref[...], 0)
    upstream = stacked_heads(do_ref[...], 1)
    bias = jnp.concatenate([bias_ref[...]] * GROUP, axis=1)
    probs = jnp.exp(matmul(pairs, queries) + bias - lse_ref[0])
    d_probs = matmul(pairs, upstream)
    center = jnp.sum(probs * d_probs, axis=0, keepdims=True)
    d_scores = (probs * (d_probs - center)).astype(jnp.bfloat16)
    d_pairs = contract_cols(d_scores, queries) + contract_cols(
        probs.astype(jnp.bfloat16), upstream
    )
    dkv_ref[...] = d_pairs.astype(jnp.bfloat16)
    d_queries = contract_rows(pairs, d_scores)
    dq_ref[...] = unstacked_heads(d_queries[:HEAD_SIZE]) * SCALE


def row_specs(rows, keys):
    place = pl.BlockSpec(memory_space=pltpu.SMEM)
    start = pl.BlockSpec((1, rows), lambda h: (0, 0))
    heads = pl.BlockSpec((rows, GROUP_WIDTH), lambda h: (0, h))
    pairs = pl.BlockSpec((keys, PAIR_WIDTH), lambda h: (0, h))
    lse = pl.BlockSpec((1, 1, GROUP * rows), lambda h: (h, 0, 0))
    return place, start, heads, pairs, lse


def attend(offsets, place, start, queries, pairs):
    rows, keys = queries.shape[0], pairs.shape[0]
    at, begin, heads, blocks, lse = row_specs(rows, keys)
    return pl.pallas_call(
        functools.partial(attend_kernel, offsets),
        grid=(KEY_VALUE_HEADS,),
        in_specs=[at, begin, heads, blocks],
        out_specs=[heads, lse],
        out_shape=[
            jax.ShapeDtypeStruct((rows, QUERY_WIDTH), jnp.bfloat16),
            jax.ShapeDtypeStruct((KEY_VALUE_HEADS, 1, GROUP * rows), jnp.float32),
        ],
        scratch_shapes=[pltpu.VMEM((keys, rows), jnp.float32)],
        cost_estimate=pl.CostEstimate(
            flops=8 * rows * keys * QUERY_WIDTH,
            bytes_accessed=4 * rows * QUERY_WIDTH + 2 * keys * KV_WIDTH,
            transcendentals=rows * keys * QUERY_HEADS,
        ),
    )(place, start, queries, pairs)


def attend_back(offsets, place, start, queries, pairs, upstream, lse_rows):
    rows, keys = queries.shape[0], pairs.shape[0]
    at, begin, heads, blocks, lse = row_specs(rows, keys)
    return pl.pallas_call(
        functools.partial(attend_back_kernel, offsets),
        grid=(KEY_VALUE_HEADS,),
        in_specs=[at, begin, heads, blocks, heads, lse],
        out_specs=[heads, blocks],
        out_shape=[
            jax.ShapeDtypeStruct((rows, QUERY_WIDTH), jnp.float32),
            jax.ShapeDtypeStruct((keys, KV_WIDTH), jnp.bfloat16),
        ],
        scratch_shapes=[pltpu.VMEM((keys, rows), jnp.float32)],
        cost_estimate=pl.CostEstimate(
            flops=20 * rows * keys * QUERY_WIDTH,
            bytes_accessed=8 * rows * QUERY_WIDTH + 4 * keys * KV_WIDTH,
            transcendentals=rows * keys * QUERY_HEADS,
        ),
    )(place, start, queries, pairs, upstream, lse_rows)


def paired(columns):
    rows = columns.shape[0]
    return (
        columns.reshape(rows, 2, KEY_VALUE_HEADS, HEAD_SIZE)
        .transpose(0, 2, 1, 3)
        .reshape(rows, KV_WIDTH)
    )


def unpaired(columns):
    rows = columns.shape[0]
    return (
        columns.reshape(rows, KEY_VALUE_HEADS, 2, HEAD_SIZE)
        .transpose(0, 2, 1, 3)
        .reshape(rows, KV_WIDTH)
    )


def per_device(
    hidden_in, w_qkv, w_out, w_gate_up, w_down, norm_gains, segment_ids, positions, out_grad
):
    row_count, rows = (hidden_in.shape[0], hidden_in.shape[1])
    dp_count, seq_count = (lax.axis_size("dp"), lax.axis_size("seq"))
    tokens = row_count * rows
    ff_part = FF // dp_count
    place = lax.axis_index("seq")
    orders = bit_orders(seq_count, row_count)
    low = jnp.bfloat16
    split = lambda array: [array[r * rows : (r + 1) * rows] for r in range(row_count)]

    here = place * rows + jnp.arange(rows, dtype=jnp.int32)
    starts = (here[None, :] - positions).reshape(row_count, 1, rows)
    place_one = place.astype(jnp.int32).reshape(1)

    with jax.named_scope("gather_qkv"):
        qkv_low = jnp.concatenate(
            [w_qkv[:, :QUERY_WIDTH], paired(w_qkv[:, QUERY_WIDTH:])], axis=1
        ).astype(low)
        w_query = lax.all_gather(qkv_low, ("dp", "seq"), axis=0, tiled=True)
    with jax.named_scope("gather_gains"):
        gains = lax.all_gather(
            norm_gains.astype(low), ("dp", "seq"), axis=0, tiled=True
        ).astype(jnp.float32)
    with jax.named_scope("swap_gate"):
        gate_rows = w_gate_up.shape[0]
        gate_blocks = (
            w_gate_up.astype(low)
            .reshape(gate_rows, 2, dp_count, ff_part)
            .transpose(2, 0, 1, 3)
            .reshape(dp_count, gate_rows, 2 * ff_part)
        )
        gate_cols = exchange_blocks(gate_blocks)
    with jax.named_scope("swap_out"):
        proj_rows = in_order(rotate_gather(w_out.astype(low)))
    with jax.named_scope("gather_out"):
        w_proj = lax.all_gather(proj_rows, "seq", axis=1, tiled=True).reshape(QUERY_WIDTH, D)
    with jax.named_scope("gather_gate"):
        w_gate = lax.all_gather(gate_cols, "seq", axis=1, tiled=True).reshape(D, 2 * ff_part)
    with jax.named_scope("gather_down"):
        w_drop = lax.all_gather(w_down.astype(low), "seq", axis=0, tiled=True)
    grad_low = out_grad.reshape(tokens, D)
    with jax.named_scope("swap_grad"):
        grad_all = [jnp.concatenate(rotate_gather(g), axis=0) for g in split(grad_low)]

    gain_one = gains[:D]
    gain_two = gains[D : 2 * D]
    gain_query = gains[2 * D : 2 * D + HEAD_SIZE]
    gain_key = gains[2 * D + HEAD_SIZE :]
    inputs = hidden_in.reshape(tokens, D).astype(jnp.float32)
    x_unit, x_scale = normalized_rows(inputs)
    normed = (x_unit * gain_one).astype(low)
    with jax.named_scope("project_qkv"):
        qkv = matmul(normed, w_query)
    cosine, sine = rope_tables(positions.reshape(tokens))
    q_unit, q_scale = normalized_rows(
        qkv[:, :QUERY_WIDTH].reshape(tokens, QUERY_HEADS, HEAD_SIZE)
    )
    kv_heads = qkv[:, QUERY_WIDTH:].reshape(tokens, KEY_VALUE_HEADS, PAIR_WIDTH)
    k_unit, k_scale = normalized_rows(kv_heads[..., :HEAD_SIZE])
    queries = apply_rotation(q_unit * gain_query, cosine, sine).astype(low).reshape(
        tokens, QUERY_WIDTH
    ) * jnp.asarray(SCALE, low)
    keys = apply_rotation(k_unit * gain_key, cosine, sine)
    kv_low = (
        jnp.concatenate([keys, kv_heads[..., HEAD_SIZE:]], axis=-1)
        .astype(low)
        .reshape(tokens, KV_WIDTH)
    )

    attended, lse, pairs, mixed, normed_two, y_unit, y_scale, normed_all = ([] for _ in range(8))
    query_rows, kv_rows, input_rows = split(queries), split(kv_low), split(inputs)
    for r in range(row_count):
        with jax.named_scope(f"gather_kv{r}"):
            pairs.append(cube_gather(kv_rows[r], orders[r]))
    for r in range(row_count):
        with jax.named_scope(f"attend{r}"):
            out_r, lse_r = attend(
                cube_offsets(orders[r]), place_one, starts[r], query_rows[r], pairs[r]
            )
        attended.append(out_r)
        lse.append(lse_r)
        with jax.named_scope(f"project_out{r}"):
            mixed.append(input_rows[r] + matmul(out_r, w_proj))
        unit_r, scale_r = normalized_rows(mixed[r])
        y_unit.append(unit_r)
        y_scale.append(scale_r)
        normed_two.append((unit_r * gain_two).astype(low))
        with jax.named_scope(f"swap_normed{r}"):
            normed_all.append(jnp.concatenate(rotate_gather(normed_two[r]), axis=0))

    hidden, d_gate_up, d_normed, block_rows = ([] for _ in range(4))
    for r in range(row_count):
        with jax.named_scope(f"back_down{r}"):
            d_hidden = contract_cols(grad_all[r], w_drop)
        with jax.named_scope(f"gate_up{r}"):
            gate_up = matmul(normed_all[r], w_gate)
        gate, up = gate_up[:, :ff_part], gate_up[:, ff_part:]
        sigmoid_gate = jax.nn.sigmoid(gate)
        silu_gate = gate * sigmoid_gate
        hidden.append((silu_gate * up).astype(low))
        d_gate = d_hidden * up * sigmoid_gate * (1.0 + gate * (1.0 - sigmoid_gate))
        d_gate_up.append(jnp.concatenate([d_gate, d_hidden * silu_gate], axis=-1).astype(low))
        with jax.named_scope(f"back_gate{r}"):
            d_partial = contract_cols(d_gate_up[r], w_gate).astype(low)
        with jax.named_scope(f"reduce_normed{r}"):
            d_normed.append(rotate_reduce(d_partial, rows))
    for r in range(row_count):
        with jax.named_scope(f"down{r}"):
            y_partial = matmul(hidden[r], w_drop).astype(low)
        with jax.named_scope(f"reduce_down{r}"):
            block_rows.append((mixed[r] + rotate_reduce(y_partial, rows)).astype(low))
    block_out = jnp.stack(block_rows)

    join = lambda parts: jnp.concatenate(parts, axis=0)
    with jax.named_scope("grad_gate"):
        gate_term = contract_rows(join(normed_all), join(d_gate_up)).astype(low)
    with jax.named_scope("grad_down"):
        down_term = contract_rows(join(hidden), join(grad_all)).astype(low)
    gate_term, down_term, *d_normed = lax.optimization_barrier((gate_term, down_term, *d_normed))
    with jax.named_scope("scatter_gate"):
        gate_sum = lax.psum_scatter(
            gate_term.reshape(dp_count, D // dp_count, 2 * ff_part),
            "seq", scatter_dimension=1, tiled=True,
        )
    with jax.named_scope("scatter_down"):
        grad_down = lax.psum_scatter(
            down_term, "seq", scatter_dimension=0, tiled=True
        ).astype(jnp.float32)
    with jax.named_scope("return_gate"):
        grad_gate_up = (
            exchange_blocks(gate_sum)
            .reshape(dp_count, gate_rows, 2, ff_part)
            .transpose(1, 2, 0, 3)
            .reshape(gate_rows, 2 * FF)
            .astype(jnp.float32)
        )

    d_mixed, d_mixed_low, d_queries, d_kv = ([] for _ in range(4))
    grad_rows = split(grad_low)
    d_gain_two = 0.0
    for r in range(row_count):
        d_gain_two = d_gain_two + jnp.sum(d_normed[r] * y_unit[r], axis=0)
        d_mixed.append(
            grad_rows[r].astype(jnp.float32)
            + normalized_gradient(d_normed[r] * gain_two, y_unit[r], y_scale[r])
        )
        d_mixed_low.append(d_mixed[r].astype(low))
        with jax.named_scope(f"back_out{r}"):
            d_attended = contract_cols(d_mixed_low[r], w_proj).astype(low)
        with jax.named_scope(f"attend_back{r}"):
            dq_r, dkv_r = attend_back(
                cube_offsets(orders[r]), place_one, starts[r], query_rows[r], pairs[r],
                d_attended, lse[r],
            )
        d_queries.append(dq_r)
        with jax.named_scope(f"reduce_kv{r}"):
            d_kv.append(cube_reduce(dkv_r, orders[r]))
    with jax.named_scope("grad_out"):
        out_term = contract_rows(join(attended), join(d_mixed_low)).astype(low)
    with jax.named_scope("scatter_out"):
        out_sum = lax.psum_scatter(
            out_term.reshape(dp_count, QUERY_WIDTH // dp_count, D),
            "seq", scatter_dimension=1, tiled=True,
        )
    with jax.named_scope("return_out"):
        grad_out = reduce_blocks(out_sum)

    d_q = apply_rotation(
        join(d_queries).reshape(tokens, QUERY_HEADS, HEAD_SIZE), cosine, -sine
    )
    d_pairs = join(d_kv).reshape(tokens, KEY_VALUE_HEADS, PAIR_WIDTH)
    d_k = apply_rotation(d_pairs[..., :HEAD_SIZE], cosine, -sine)
    d_gain_query = jnp.sum(d_q * q_unit, axis=(0, 1))
    d_gain_key = jnp.sum(d_k * k_unit, axis=(0, 1))
    d_q_raw = normalized_gradient(d_q * gain_query, q_unit, q_scale).reshape(tokens, QUERY_WIDTH)
    d_k_raw = normalized_gradient(d_k * gain_key, k_unit, k_scale)
    d_kv_raw = jnp.concatenate([d_k_raw, d_pairs[..., HEAD_SIZE:]], axis=-1).reshape(
        tokens, KV_WIDTH
    )
    d_qkv = jnp.concatenate([d_q_raw, d_kv_raw], axis=-1).astype(low)
    with jax.named_scope("grad_qkv"):
        qkv_term = contract_rows(normed, d_qkv).astype(low)
    with jax.named_scope("scatter_qkv"):
        qkv_sum = lax.psum_scatter(
            qkv_term.reshape(dp_count, D // dp_count, QUERY_WIDTH + KV_WIDTH),
            "seq", scatter_dimension=1, tiled=True,
        )
    with jax.named_scope("return_qkv"):
        qkv_own = reduce_blocks(qkv_sum)
    grad_qkv = jnp.concatenate(
        [qkv_own[:, :QUERY_WIDTH], unpaired(qkv_own[:, QUERY_WIDTH:])], axis=1
    )
    with jax.named_scope("back_qkv"):
        d_first = contract_cols(d_qkv, w_query)
    d_gain_one = jnp.sum(d_first * x_unit, axis=0)
    d_inputs = join(d_mixed) + normalized_gradient(d_first * gain_one, x_unit, x_scale)
    in_grad = d_inputs.astype(low).reshape(row_count, rows, D)

    with jax.named_scope("reduce_gains"):
        gain_term = jnp.concatenate([d_gain_one, d_gain_two, d_gain_query, d_gain_key])
        gain_term = gain_term.reshape(dp_count, seq_count, -1)
        for bit in orders[0]:
            gain_term = gain_term + crossed(gain_term, bit)
        grad_gains = lax.dynamic_index_in_dim(reduce_blocks(gain_term), place, 0, keepdims=False)
    return (
        block_out, in_grad, grad_qkv, grad_out, grad_gate_up, grad_down, grad_gains
    )


def solution(mesh):
    both = ("dp", "seq")
    return jax.shard_map(
        per_device,
        mesh=mesh,
        in_specs=(
            P("dp", "seq", None),
            P(both, None),
            P(both, None),
            P(both, None),
            P(both, None),
            P(both),
            P("dp", "seq"),
            P("dp", "seq"),
            P("dp", "seq", None),
        ),
        out_specs=(
            P("dp", "seq", None),
            P("dp", "seq", None),
            P(both, None),
            P(both, None),
            P(both, None),
            P(both, None),
            P(both),
        ),
        check_vma=False,
    )
```

```python
import functools

import jax
import jax.numpy as jnp
from jax import lax
from jax.experimental import pallas as pl
from jax.experimental.pallas import tpu as pltpu
from jax.sharding import PartitionSpec as P


D = 2048
QUERY_HEADS = 20
KEY_VALUE_HEADS = 5
HEAD_SIZE = 64
FF = 8192
GROUP = QUERY_HEADS // KEY_VALUE_HEADS
QUERY_WIDTH = QUERY_HEADS * HEAD_SIZE
PAIR_WIDTH = 2 * HEAD_SIZE
KV_WIDTH = KEY_VALUE_HEADS * PAIR_WIDTH
GROUP_WIDTH = GROUP * HEAD_SIZE

EPSILON = 1e-06
MASKED = -1e30
SCALE = HEAD_SIZE ** (-0.5)


def normalized_rows(values):
    scale_rows = lax.rsqrt(jnp.mean(values * values, axis=-1, keepdims=True) + EPSILON)
    return (values * scale_rows, scale_rows)


def normalized_gradient(upstream, unit_vals, scale_rows):
    return scale_rows * (
        upstream - unit_vals * jnp.mean(upstream * unit_vals, axis=-1, keepdims=True)
    )


def rope_tables(positions):
    freq = 1.0 / 10000.0 ** (jnp.arange(0, HEAD_SIZE, 2).astype(jnp.float32) / HEAD_SIZE)
    angle = positions.astype(jnp.float32)[:, None, :] * freq[None, :, None]
    return jnp.stack([jnp.cos(angle), jnp.sin(angle)], axis=1)


def matmul(left, right):
    return jnp.dot(left, right, preferred_element_type=jnp.float32)


def contract_rows(left, right):
    return lax.dot_general(
        left, right, (((0,), (0,)), ((), ())), preferred_element_type=jnp.float32
    )


def contract_cols(left, right):
    return lax.dot_general(
        left, right, (((1,), (1,)), ((), ())), preferred_element_type=jnp.float32
    )


def shifted(piece, shift):
    count = lax.axis_size("dp")
    return lax.ppermute(piece, "dp", [(i, (i + shift) % count) for i in range(count)])


def rotate_gather(piece):
    return [piece] + [shifted(piece, s) for s in range(1, lax.axis_size("dp"))]


def line_gather(piece):
    count = lax.axis_size("dp")
    me = lax.axis_index("dp")
    up, down, ups, downs = piece, piece, [], []
    for hop in range(1, count):
        up = lax.ppermute(up, "dp", [(i, i + 1) for i in range(hop - 1, count - 1)])
        down = lax.ppermute(down, "dp", [(i, i - 1) for i in range(1, count + 1 - hop)])
        ups.append(up)
        downs.append(down)
    return [piece] + [
        jnp.where(me >= s, ups[s - 1], downs[count - s - 1]) for s in range(1, count)
    ]


def rotate_slots(partial, rows):
    return [partial[:rows]] + [
        shifted(partial[s * rows : (s + 1) * rows].astype(jnp.bfloat16), -s)
        for s in range(1, lax.axis_size("dp"))
    ]


def line_reduce(partial, rows):
    count = lax.axis_size("dp")
    slots = [partial[s * rows : (s + 1) * rows] for s in range(count)]
    up, down = slots[1], slots[count - 1]
    for hop in range(1, count):
        if hop > 1:
            up = (slots[hop].astype(jnp.float32) + up.astype(jnp.float32)).astype(jnp.bfloat16)
            down = (slots[count - hop].astype(jnp.float32) + down.astype(jnp.float32)).astype(
                jnp.bfloat16
            )
        up = lax.ppermute(up, "dp", [(i, i + 1) for i in range(hop)])
        down = lax.ppermute(down, "dp", [(i, i - 1) for i in range(count - hop, count)])
    return added([slots[0], up, down])


def added(slots):
    return functools.reduce(jnp.add, [slot.astype(jnp.float32) for slot in slots])


def in_order(slots):
    count = len(slots)
    back = slots[::-1] + slots[::-1]
    start = count - 1 - lax.axis_index("dp")
    return lax.dynamic_slice_in_dim(jnp.stack(back[:-1]), start, count, axis=0)


def exchange_blocks(pick):
    count = lax.axis_size("dp")
    me = lax.axis_index("dp")
    return in_order([pick(me)] + [shifted(pick(lax.rem(me + s, count)), s) for s in range(1, count)])


def reduce_blocks(blocks):
    count = lax.axis_size("dp")
    me = lax.axis_index("dp")
    pick = lambda s: lax.dynamic_index_in_dim(blocks, lax.rem(me + s, count), 0, keepdims=False)
    total = pick(0).astype(jnp.float32)
    for s in range(1, count):
        total = total + shifted(pick(s), s).astype(jnp.float32)
    return total


def bit_orders(count, ways):
    bits = [1 << i for i in range(1, count.bit_length() - 1)]
    half = (len(bits) + 1) // 2
    low, high = bits[:half], bits[half:]
    orders = []
    for way in range(ways):
        one, two = (low, high) if way % 2 == 0 else (high, low)
        order = []
        for i in range(half):
            order += one[i : i + 1] + two[i : i + 1]
        orders.append(tuple(order + [1]))
    return orders


def crossed(piece, bit):
    count = lax.axis_size("seq")
    return lax.ppermute(piece, "seq", [(i, i ^ bit) for i in range(count)])


def cube_gather(piece, bits):
    for bit in bits:
        other = crossed(piece, bit)
        piece = jnp.concatenate([piece, other], axis=0)
    return piece


def cube_gather_in_order(piece):
    bit = 1
    while bit < lax.axis_size("seq"):
        other = crossed(piece, bit)
        upper = (lax.axis_index("seq") & bit) > 0
        piece = jnp.where(
            upper, jnp.concatenate([other, piece]), jnp.concatenate([piece, other])
        )
        bit *= 2
    return piece


def cube_offsets(bits):
    offsets = [0]
    for bit in bits:
        offsets = offsets + [o ^ bit for o in offsets]
    return tuple(offsets)


def cube_reduce(partial, bits):
    for bit in bits[::-1]:
        half = partial.shape[0] // 2
        other = crossed(partial[half:].astype(jnp.bfloat16), bit)
        partial = partial[:half].astype(jnp.float32) + other.astype(jnp.float32)
    return partial


def cube_scatter(term, bits):
    me = lax.axis_index("seq")
    left = sorted(bits)
    for bit in bits[::-1]:
        low_count = 1 << left.index(bit)
        left.remove(bit)
        lead, _, *rest = term.shape
        view = term.reshape(lead, -1, 2, low_count, *rest)
        mine = jnp.minimum(me & bit, 1)
        pick = lambda i: lax.dynamic_index_in_dim(view, i, 2, keepdims=False).reshape(
            lead, -1, *rest
        )
        other = crossed(pick(1 - mine).astype(jnp.bfloat16), bit)
        term = pick(mine).astype(jnp.float32) + other.astype(jnp.float32)
    return term[:, 0]


def halves_scatter(term, orders):
    half = term.shape[0] // 2
    return jnp.concatenate(
        [cube_scatter(term[:half], orders[0]), cube_scatter(term[half:], orders[1])]
    ).astype(jnp.bfloat16)


def fill_bias(place_ref, start_ref, bias_ref, offsets):
    rows = start_ref.shape[1]
    place = place_ref[0]
    query = place * rows + lax.broadcasted_iota(jnp.int32, (rows, rows), 1)
    begin = start_ref[...]
    local = lax.broadcasted_iota(jnp.int32, (rows, rows), 0)
    for slot, offset in enumerate(offsets):
        key = (place ^ offset) * rows + local
        allowed = (key <= query) & (key >= begin)
        bias_ref[slot * rows : (slot + 1) * rows, :] = jnp.where(allowed, 0.0, MASKED)


def unstacked_heads(turned):
    rows = turned.shape[1] // GROUP
    return jnp.concatenate([turned[:, g * rows : (g + 1) * rows] for g in range(GROUP)], axis=0).T


def each_row(offsets, place_ref, start_ref, bias_ref):
    for r, order in enumerate(offsets):

        @pl.when((pl.program_id(0) == r) & (pl.program_id(1) == 0))
        def _():
            fill_bias(place_ref, start_ref, bias_ref, order)


def side_by_side(block):
    turned = block.astype(jnp.float32).T
    return jnp.concatenate(
        [turned[g * HEAD_SIZE : (g + 1) * HEAD_SIZE] for g in range(GROUP)], axis=1
    )


def unit_columns(values):
    scale = lax.rsqrt(jnp.mean(values * values, axis=0, keepdims=True) + EPSILON)
    return values * scale, scale


def turn_columns(values, cosine, sine):
    half = HEAD_SIZE // 2
    first, second = values[:half], values[half:]
    return jnp.concatenate(
        [first * cosine - second * sine, second * cosine + first * sine], axis=0
    )


def raw_gradient(upstream, unit, scale, gain, cosine, sine):
    straight = turn_columns(upstream, cosine, -sine)
    gained = straight * gain
    center = jnp.mean(gained * unit, axis=0, keepdims=True)
    return scale * (gained - unit * center), straight * unit


def prepared(block, gain, tables, heads):
    cosine = jnp.concatenate([tables[0]] * heads, axis=1)
    sine = jnp.concatenate([tables[1]] * heads, axis=1)
    unit, scale = unit_columns(block)
    return unit, scale, cosine, sine, turn_columns(unit * gain, cosine, sine)


def padded(heads, place):
    empty = jnp.zeros(heads.shape, jnp.bfloat16)
    return jnp.concatenate([heads, empty] if place == 0 else [empty, heads], axis=0)


def rounded_queries(turned):
    return padded((turned.astype(jnp.bfloat16).astype(jnp.float32) * SCALE).astype(jnp.bfloat16), 0)


def attend_kernel(
    offsets, place_ref, start_ref, gain_ref, table_ref, q_ref, kv_ref, out_ref, lse_ref, bias_ref
):
    each_row(offsets, place_ref, start_ref.at[0], bias_ref)
    pairs = kv_ref[...]
    block = side_by_side(q_ref[...])
    queries = rounded_queries(prepared(block, gain_ref[...], table_ref[0], GROUP)[-1])
    bias = jnp.concatenate([bias_ref[...]] * GROUP, axis=1)
    scores = matmul(pairs, queries) + bias
    peak = jnp.max(scores, axis=0, keepdims=True)
    raised = jnp.exp(scores - peak)
    totals = jnp.sum(raised, axis=0, keepdims=True)
    probs = (raised * (1.0 / totals)).astype(jnp.bfloat16)
    mixed = contract_rows(pairs, probs)
    out_ref[...] = unstacked_heads(mixed[HEAD_SIZE:]).astype(jnp.bfloat16)
    lse_ref[0, 0] = peak + jnp.log(totals)


def attend_back_kernel(
    offsets, place_ref, start_ref, gain_ref, table_ref, q_ref, kv_ref, do_ref, lse_ref,
    dq_ref, dkv_ref, dgain_ref, bias_ref,
):
    each_row(offsets, place_ref, start_ref.at[0], bias_ref)
    pairs = kv_ref[...]
    gain = gain_ref[...]
    unit, scale, cosine, sine, turned = prepared(
        side_by_side(q_ref[...]), gain, table_ref[0], GROUP
    )
    queries = rounded_queries(turned)
    upstream = padded(side_by_side(do_ref[...]).astype(jnp.bfloat16), 1)
    bias = jnp.concatenate([bias_ref[...]] * GROUP, axis=1)
    probs = jnp.exp(matmul(pairs, queries) + bias - lse_ref[0, 0])
    d_probs = matmul(pairs, upstream)
    center = jnp.sum(probs * d_probs, axis=0, keepdims=True)
    d_scores = (probs * (d_probs - center)).astype(jnp.bfloat16)
    d_pairs = contract_cols(d_scores, queries) + contract_cols(
        probs.astype(jnp.bfloat16), upstream
    )
    dkv_ref[...] = d_pairs.astype(jnp.bfloat16)
    d_queries = contract_rows(pairs, d_scores)[:HEAD_SIZE] * SCALE
    d_raw, d_gain = raw_gradient(d_queries, unit, scale, gain, cosine, sine)
    dq_ref[...] = unstacked_heads(d_raw).astype(jnp.bfloat16)

    @pl.when((pl.program_id(0) == 0) & (pl.program_id(1) == 0))
    def _():
        dgain_ref[...] = jnp.zeros_like(dgain_ref)

    rows = dgain_ref.shape[1]
    for g in range(GROUP):
        dgain_ref[...] += d_gain[:, g * rows : (g + 1) * rows]


def keys_kernel(gain_ref, table_ref, kv_ref, out_ref):
    turned = kv_ref[...].T
    keys = prepared(turned[:HEAD_SIZE], gain_ref[...], table_ref, 1)[-1]
    out_ref[...] = jnp.concatenate([keys, turned[HEAD_SIZE:]], axis=0).T.astype(jnp.bfloat16)


def keys_back_kernel(gain_ref, table_ref, kv_ref, d_ref, out_ref, dgain_ref):
    gain = gain_ref[...]
    unit, scale, cosine, sine, _ = prepared(kv_ref[...].T[:HEAD_SIZE], gain, table_ref, 1)
    upstream = d_ref[...].T
    d_raw, d_gain = raw_gradient(upstream[:HEAD_SIZE], unit, scale, gain, cosine, sine)
    out_ref[...] = jnp.concatenate([d_raw, upstream[HEAD_SIZE:]], axis=0).T.astype(jnp.bfloat16)

    @pl.when(pl.program_id(0) == 0)
    def _():
        dgain_ref[...] = jnp.zeros_like(dgain_ref)

    dgain_ref[...] += d_gain


def row_specs(rows, keys):
    whole = lambda shape: pl.BlockSpec(shape, lambda r, h: (0,) * len(shape))
    return (
        pl.BlockSpec(memory_space=pltpu.SMEM),
        pl.BlockSpec((1, 1, rows), lambda r, h: (r, 0, 0)),
        whole((HEAD_SIZE, 1)),
        pl.BlockSpec((1, 2, HEAD_SIZE // 2, rows), lambda r, h: (r, 0, 0, 0)),
        pl.BlockSpec((rows, GROUP_WIDTH), lambda r, h: (r, h)),
        pl.BlockSpec((keys, PAIR_WIDTH), lambda r, h: (r, h)),
        pl.BlockSpec((1, 1, 1, GROUP * rows), lambda r, h: (r, h, 0, 0)),
        whole((HEAD_SIZE, rows)),
    )


def attend(offsets, place, start, gain, tables, qkv, pairs):
    count = len(offsets)
    rows, keys = qkv.shape[0] // count, pairs.shape[0] // count
    at, begin, gains, turns, heads, blocks, lse, _ = row_specs(rows, keys)
    return pl.pallas_call(
        functools.partial(attend_kernel, offsets),
        grid=(count, KEY_VALUE_HEADS),
        in_specs=[at, begin, gains, turns, heads, blocks],
        out_specs=[heads, lse],
        out_shape=[
            jax.ShapeDtypeStruct((count * rows, QUERY_WIDTH), jnp.bfloat16),
            jax.ShapeDtypeStruct((count, KEY_VALUE_HEADS, 1, GROUP * rows), jnp.float32),
        ],
        scratch_shapes=[pltpu.VMEM((keys, rows), jnp.float32)],
        cost_estimate=pl.CostEstimate(
            flops=8 * count * rows * keys * QUERY_WIDTH,
            bytes_accessed=count * (6 * rows * QUERY_WIDTH + 2 * keys * KV_WIDTH),
            transcendentals=count * rows * keys * QUERY_HEADS,
        ),
    )(place, start, gain, tables, qkv, pairs)


def attend_back(offsets, place, start, gain, tables, qkv, pairs, upstream, lse_rows):
    count = len(offsets)
    rows, keys = qkv.shape[0] // count, pairs.shape[0] // count
    at, begin, gains, turns, heads, blocks, lse, sums = row_specs(rows, keys)
    return pl.pallas_call(
        functools.partial(attend_back_kernel, offsets),
        grid=(count, KEY_VALUE_HEADS),
        in_specs=[at, begin, gains, turns, heads, blocks, heads, lse],
        out_specs=[heads, blocks, sums],
        out_shape=[
            jax.ShapeDtypeStruct((count * rows, QUERY_WIDTH), jnp.bfloat16),
            jax.ShapeDtypeStruct((count * keys, KV_WIDTH), jnp.bfloat16),
            jax.ShapeDtypeStruct((HEAD_SIZE, rows), jnp.float32),
        ],
        scratch_shapes=[pltpu.VMEM((keys, rows), jnp.float32)],
        cost_estimate=pl.CostEstimate(
            flops=20 * count * rows * keys * QUERY_WIDTH,
            bytes_accessed=count * (8 * rows * QUERY_WIDTH + 4 * keys * KV_WIDTH),
            transcendentals=count * rows * keys * QUERY_HEADS,
        ),
    )(place, start, gain, tables, qkv, pairs, upstream, lse_rows)


def keys_specs(tokens):
    first = QUERY_WIDTH // PAIR_WIDTH
    return (
        pl.BlockSpec((HEAD_SIZE, 1), lambda h: (0, 0)),
        pl.BlockSpec((2, HEAD_SIZE // 2, tokens), lambda h: (0, 0, 0)),
        pl.BlockSpec((tokens, PAIR_WIDTH), lambda h: (0, first + h)),
        pl.BlockSpec((tokens, PAIR_WIDTH), lambda h: (0, h)),
        pl.BlockSpec((HEAD_SIZE, tokens), lambda h: (0, 0)),
    )


def keys_forward(gain, tables, qkv):
    tokens = qkv.shape[0]
    gains, turns, raw, own, _ = keys_specs(tokens)
    return pl.pallas_call(
        keys_kernel,
        grid=(KEY_VALUE_HEADS,),
        in_specs=[gains, turns, raw],
        out_specs=own,
        out_shape=jax.ShapeDtypeStruct((tokens, KV_WIDTH), jnp.bfloat16),
        cost_estimate=pl.CostEstimate(
            flops=20 * tokens * KV_WIDTH, bytes_accessed=6 * tokens * KV_WIDTH, transcendentals=0
        ),
    )(gain, tables, qkv)


def keys_back(gain, tables, qkv, upstream):
    tokens = qkv.shape[0]
    gains, turns, raw, own, sums = keys_specs(tokens)
    return pl.pallas_call(
        keys_back_kernel,
        grid=(KEY_VALUE_HEADS,),
        in_specs=[gains, turns, raw, own],
        out_specs=[own, sums],
        out_shape=[
            jax.ShapeDtypeStruct((tokens, KV_WIDTH), jnp.bfloat16),
            jax.ShapeDtypeStruct((HEAD_SIZE, tokens), jnp.float32),
        ],
        cost_estimate=pl.CostEstimate(
            flops=40 * tokens * KV_WIDTH, bytes_accessed=10 * tokens * KV_WIDTH, transcendentals=0
        ),
    )(gain, tables, qkv, upstream)


def paired(columns):
    rows = columns.shape[0]
    return (
        columns.reshape(rows, 2, KEY_VALUE_HEADS, HEAD_SIZE)
        .transpose(0, 2, 1, 3)
        .reshape(rows, KV_WIDTH)
    )


def unpaired(columns):
    rows = columns.shape[0]
    return (
        columns.reshape(rows, KEY_VALUE_HEADS, 2, HEAD_SIZE)
        .transpose(0, 2, 1, 3)
        .reshape(rows, KV_WIDTH)
    )


def per_device(
    hidden_in, w_qkv, w_out, w_gate_up, w_down, norm_gains, segment_ids, positions, out_grad
):
    row_count, rows = (hidden_in.shape[0], hidden_in.shape[1])
    dp_count, seq_count = (lax.axis_size("dp"), lax.axis_size("seq"))
    tokens = row_count * rows
    ff_part = FF // dp_count
    place = lax.axis_index("seq")
    orders = bit_orders(seq_count, row_count)
    low = jnp.bfloat16
    split = lambda array: [array[r * rows : (r + 1) * rows] for r in range(row_count)]

    here = place * rows + jnp.arange(rows, dtype=jnp.int32)
    starts = (here[None, :] - positions).reshape(row_count, 1, rows)
    place_one = place.astype(jnp.int32).reshape(1)

    gains_seq = cube_gather_in_order(norm_gains.astype(low))
    gains = in_order(rotate_gather(gains_seq)).reshape(-1).astype(jnp.float32)
    qkv_low = jnp.concatenate(
        [w_qkv[:, :QUERY_WIDTH], paired(w_qkv[:, QUERY_WIDTH:])], axis=1
    ).astype(low)
    qkv_rows = in_order(rotate_gather(qkv_low))
    w_query = lax.all_gather(qkv_rows, "seq", axis=1, tiled=True).reshape(D, -1)
    proj_rows = in_order(rotate_gather(w_out.astype(low)))
    part = lambda start: lax.dynamic_slice_in_dim(w_gate_up, start, ff_part, axis=1)
    gate_cols = exchange_blocks(
        lambda d: jnp.concatenate([part(d * ff_part), part(FF + d * ff_part)], axis=1).astype(low)
    )
    w_proj = lax.all_gather(proj_rows, "seq", axis=1, tiled=True).reshape(QUERY_WIDTH, D)
    w_gate = lax.all_gather(gate_cols, "seq", axis=1, tiled=True).reshape(D, 2 * ff_part)
    w_drop = lax.all_gather(w_down.astype(low), "seq", axis=0, tiled=True)
    grad_low = out_grad.reshape(tokens, D)
    grad_all = jnp.concatenate(line_gather(grad_low), axis=0)

    gain_one = gains[:D]
    gain_two = gains[D : 2 * D]
    gain_query = gains[2 * D : 2 * D + HEAD_SIZE]
    gain_key = gains[2 * D + HEAD_SIZE :]
    inputs = hidden_in.reshape(tokens, D).astype(jnp.float32)
    x_unit, x_scale = normalized_rows(inputs)
    normed = (x_unit * gain_one).astype(low)
    qkv = matmul(normed, w_query)
    tables = rope_tables(positions)
    flat_tables = tables.transpose(1, 2, 0, 3).reshape(2, HEAD_SIZE // 2, tokens)
    query_column, key_column = gain_query[:, None], gain_key[:, None]
    kv_low = keys_forward(key_column, flat_tables, qkv)

    pairs = []
    for r, kv_row in enumerate(split(kv_low)):
        pairs.append(cube_gather(kv_row, orders[r]))
    offsets = tuple(cube_offsets(order) for order in orders)
    pairs = jnp.concatenate(pairs, axis=0)
    attended, lse = attend(
        offsets, place_one, starts, query_column, tables, qkv, pairs
    )
    mixed = inputs + matmul(attended, w_proj)
    y_unit, y_scale = normalized_rows(mixed)
    mixed, y_scale, normed_two = lax.optimization_barrier(
        (mixed, y_scale, (y_unit * gain_two).astype(low))
    )
    normed_all = jnp.concatenate(line_gather(normed_two), axis=0)

    gate_up = matmul(normed_all, w_gate)
    d_hidden = contract_cols(grad_all, w_drop)
    gate, up = gate_up[:, :ff_part], gate_up[:, ff_part:]
    sigmoid_gate = jax.nn.sigmoid(gate)
    silu_gate = gate * sigmoid_gate
    hidden = (silu_gate * up).astype(low)
    d_gate = d_hidden * up * sigmoid_gate * (1.0 + gate * (1.0 - sigmoid_gate))
    d_gate_up = jnp.concatenate([d_gate, d_hidden * silu_gate], axis=-1).astype(low)
    d_partial = contract_cols(d_gate_up, w_gate).astype(low)
    d_normed = line_reduce(d_partial, tokens)
    gate_term = contract_rows(normed_all, d_gate_up).astype(low)
    down_term = contract_rows(hidden, grad_all).astype(low)
    y_partial = matmul(hidden, w_drop).astype(low)
    y_slots = rotate_slots(y_partial, tokens)
    gate_sum = lax.psum_scatter(
        gate_term.reshape(dp_count, D // dp_count, 2 * ff_part),
        "seq", scatter_dimension=1, tiled=True,
    )
    blocks = down_term.reshape(1, seq_count, -1, D)
    half = blocks.shape[2] // 2
    grad_down = jnp.concatenate(
        [
            cube_scatter(part, order)[0]
            for part, order in zip(
                (blocks[:, :, :half], blocks[:, :, half:]), bit_orders(seq_count, 2)
            )
        ]
    )
    gate_own = exchange_blocks(lambda d: lax.dynamic_index_in_dim(gate_sum, d, 0, keepdims=False))
    grad_gate_up = jnp.concatenate(
        [gate_own[d, :, :ff_part] for d in range(dp_count)]
        + [gate_own[d, :, ff_part:] for d in range(dp_count)],
        axis=1,
    ).astype(jnp.float32)

    d_mixed = grad_low.astype(jnp.float32) + normalized_gradient(
        d_normed * gain_two, mixed * y_scale, y_scale
    )
    d_mixed, d_mixed_low, d_normed = lax.optimization_barrier(
        (d_mixed, d_mixed.astype(low), d_normed)
    )
    d_attended = contract_cols(d_mixed_low, w_proj).astype(low)
    out_term = contract_rows(attended, d_mixed_low).astype(low)
    d_q_raw, d_pairs, query_sums = attend_back(
        offsets, place_one, starts, query_column, tables, qkv, pairs, d_attended, lse
    )
    d_kv = []
    for r, d_row in enumerate(jnp.split(d_pairs, row_count)):
        d_kv.append(cube_reduce(d_row, orders[r]))
    out_sum = halves_scatter(out_term.reshape(dp_count, seq_count, -1, D), bit_orders(seq_count, 2))
    grad_out = reduce_blocks(out_sum)

    d_kv_raw, key_sums = keys_back(key_column, flat_tables, qkv, jnp.concatenate(d_kv))
    d_qkv = jnp.concatenate([d_q_raw, d_kv_raw], axis=-1)
    late_mixed, y_scale, d_normed = late((mixed, y_scale, d_normed), d_q_raw)
    d_gain_two = jnp.sum(d_normed * (late_mixed * y_scale), axis=0)
    qkv_term = contract_rows(normed, d_qkv).astype(low)
    d_first = contract_cols(d_qkv, w_query)
    d_gain_one = jnp.sum(d_first * x_unit, axis=0)
    d_inputs = late(d_mixed, qkv_term) + normalized_gradient(d_first * gain_one, x_unit, x_scale)
    in_grad = d_inputs.astype(low).reshape(row_count, rows, D)
    gain_term = jnp.concatenate(
        [d_gain_one, d_gain_two, jnp.sum(query_sums, axis=1), jnp.sum(key_sums, axis=1)]
    ).astype(low)
    qkv_rows, gain_count = D // dp_count // seq_count, norm_gains.shape[0]
    block = jnp.concatenate(
        [
            qkv_term.reshape(dp_count, seq_count, qkv_rows, -1),
            jnp.pad(
                gain_term.reshape(dp_count, seq_count, 1, gain_count),
                ((0, 0), (0, 0), (0, 7), (0, QUERY_WIDTH + KV_WIDTH - gain_count)),
            ),
        ],
        axis=2,
    )
    qkv_sum = halves_scatter(block, bit_orders(seq_count, 2))
    y_slots, mixed = late((y_slots, mixed), qkv_term)
    block_out = (mixed + added(y_slots)).astype(low).reshape(row_count, rows, D)
    qkv_own = reduce_blocks(qkv_sum)
    grad_gains = qkv_own[qkv_rows, :gain_count]
    grad_qkv = jnp.concatenate(
        [qkv_own[:qkv_rows, :QUERY_WIDTH], unpaired(qkv_own[:qkv_rows, QUERY_WIDTH:])], axis=1
    )
    return (
        block_out, in_grad, grad_qkv, grad_out, grad_gate_up, grad_down, grad_gains
    )


def late(values, anchor):
    return lax.optimization_barrier((values, anchor))[0]


def solution(mesh):
    both = ("dp", "seq")
    return jax.shard_map(
        per_device,
        mesh=mesh,
        in_specs=(
            P("dp", "seq", None),
            P(both, None),
            P(both, None),
            P(both, None),
            P(both, None),
            P(both),
            P("dp", "seq"),
            P("dp", "seq"),
            P("dp", "seq", None),
        ),
        out_specs=(
            P("dp", "seq", None),
            P("dp", "seq", None),
            P(both, None),
            P(both, None),
            P(both, None),
            P(both, None),
            P(both),
        ),
        check_vma=False,
    )
```
